256 devices in a mesh: groups: 2 (over y), ep: 128 (over x, z, core).
Axes of the slice: x: 4, y: 2, z: 16, core: 2. Of those that a mesh axis runs over, the one named last changes fastest.
The devices are a block of a 4x16x16 slice.
Arguments:
- tokens: bfloat16 [32768, 1440], P(('groups', 'ep')), parts along dimension 0, may hold values from -6 to 6
- expert_ids: int32 [32768, 4], P(('groups', 'ep')), parts along dimension 0, may hold values from 0 to 127, as said below
- combine: float32 [32768, 4], P(('groups', 'ep')), parts along dimension 0, may hold values from 0.05 to 1
- gate_weight: bfloat16 [128, 1440, 1440], P('ep'), may hold values from -0.15625 to 0.15625
- up_weight: bfloat16 [128, 1440, 1440], P('ep'), may hold values from -0.15625 to 0.15625
- down_weight: bfloat16 [128, 1440, 1440], P('ep'), may hold values from -0.15625 to 0.15625
Outputs:
- mixture: bfloat16 [32768, 1440], P(('groups', 'ep')), parts along dimension 0
The draws below stay inside these ranges and needn't reach their ends.
There are 2 independent parts, one for each index of `groups`. The reference program is written for one: setup_inputs(seed, part) draws one part's arguments, and reference() takes and returns one part's arrays. A program takes and returns all parts, laid end to end along the dimension named above; an argument that names none is the same for every part. Nothing has to cross between parts.
Inputs may be any that keep to these rules, and one draw needn't show every extreme that they name: `expert_ids`: each row names 4 different experts. In the rows of one device (aligned blocks of 128 rows) no expert is named more than 8 times, and some expert is named exactly 8 times in every block.
All inputs are finite; a program needn't handle non-finite values.
Results may differ from the reference program's by a relative error of at most 0.0058.
Values may be sent and summed in bfloat16 or wider, within the bound.
A program may use at most 64 MiB of HBM per device.

```python
import math
import jax
import jax.numpy as jnp
from jax import lax

D = 1440
FF = 1440
TOP = 4
TOK_DEV = 128
EXPERTS = 128
TOKENS = 16384
CAP = 8
N_EP = 128


def route_block(key, ranking):
    cells = EXPERTS * CAP
    expert_of_cell = jnp.arange(cells, dtype=jnp.int32) // CAP
    position_in_expert = ranking[expert_of_cell]
    routing_boost = (4 << 20) // (position_in_expert + 1)
    random_jitter = jax.random.randint(jax.random.fold_in(key, 1), (cells,), 0, 1 << 20, dtype=jnp.int32)
    router_logits = routing_boost + random_jitter
    chosen = jnp.argsort(-router_logits, stable=True)[:TOK_DEV * TOP]
    listed = jnp.sort(expert_of_cell[chosen])
    table = listed.reshape(TOP, TOK_DEV).T
    random_reorder = jax.random.permutation(jax.random.fold_in(key, 2), TOK_DEV)
    return table[random_reorder]


def draw_expert_ids(key, part):
    ranking = jax.random.permutation(jax.random.fold_in(key, 7), EXPERTS).astype(jnp.int32)

    def one_block(index):
        return route_block(jax.random.fold_in(key, 100 + index), ranking)
    blocks = jax.vmap(one_block)(jnp.arange(N_EP, dtype=jnp.int32))
    return blocks.reshape(TOKENS, TOP).astype(jnp.int32)


def steps_of(own_key, dims, split, low, top_value):
    def one(axis_at, blocks):
        draws = jax.random.uniform(jax.random.fold_in(jax.random.fold_in(own_key, 6), axis_at), (blocks,), jnp.float32, low / len(split), top_value / len(split))
        return jnp.repeat(jnp.exp(draws), dims[axis_at] // blocks).reshape((-1,) + (1,) * (len(dims) - axis_at - 1))

    level = one(*split[0])
    for cut in split[1:]:
        level = level * one(*cut)
    return level


def bell_draw(key, extent, spread, reach, cuts=(), kind=jnp.bfloat16):
    entries = spread * jax.random.normal(key, extent, jnp.float32)
    if cuts:
        entries = entries * steps_of(key, extent, cuts, -0.22, 0.18)
    return jnp.clip(entries, -reach, reach).astype(kind)


def setup_inputs(seed: int = 0, part: int = 0) -> dict:
    arg_keys = jax.random.split(jax.random.key(seed), 7)
    own_keys = jax.random.split(jax.random.fold_in(arg_keys[6], part), 7)
    tokens = bell_draw(own_keys[0], (TOKENS, D), 1.0, 6.0, ((0, 128),))
    expert_ids = draw_expert_ids(jax.random.fold_in(jax.random.fold_in(arg_keys[6], part), 71), part)
    combine = jnp.clip(jnp.exp(math.log(1.0) - 2.9957323 * jax.random.uniform(own_keys[2], (TOKENS, TOP), jnp.float32) ** steps_of(own_keys[2], (TOKENS, TOP), ((0, 128),), -0.2, 0.2)), 0.05, 1.0)
    gate_weight = bell_draw(arg_keys[3], (EXPERTS, D, FF), D ** -0.5, 0.15625, ((0, 128),))
    up_weight = bell_draw(arg_keys[4], (EXPERTS, D, FF), D ** -0.5, 0.15625, ((0, 128),))
    down_weight = bell_draw(arg_keys[5], (EXPERTS, FF, D), FF ** -0.5, 0.15625, ((0, 128),))
    return dict(tokens=tokens, expert_ids=expert_ids, combine=combine, gate_weight=gate_weight, up_weight=up_weight, down_weight=down_weight)


alpha_gate = 1.702


def run_expert_block(row_block, gate_proj, up_proj, down_proj):
    gate_part = jnp.dot(row_block, gate_proj, preferred_element_type=jnp.float32)
    up_part = jnp.dot(row_block, up_proj, preferred_element_type=jnp.float32)
    hidden = ((up_part + 1.0) * gate_part * jax.nn.sigmoid(alpha_gate * gate_part)).astype(jnp.bfloat16)
    return jnp.dot(hidden, down_proj, preferred_element_type=jnp.float32).astype(jnp.bfloat16)


def reference(tokens, expert_ids, combine, gate_weight, up_weight, down_weight):
    most_rows = N_EP * CAP

    def per_expert(carry, inputs):
        expert, gate_proj, up_proj, down_proj = inputs
        chosen = expert_ids == expert
        weight_row = jnp.sum(jnp.where(chosen, combine, jnp.zeros_like(combine)), axis=1)
        present = jnp.any(chosen, axis=1)
        indices = jnp.nonzero(present, size=most_rows, fill_value=0)[0].astype(jnp.int32)
        valid = jnp.arange(most_rows, dtype=jnp.int32) < jnp.sum(present.astype(jnp.int32))
        outputs = run_expert_block(tokens[indices], gate_proj, up_proj, down_proj)
        factor = jnp.where(valid, weight_row[indices], jnp.zeros_like(weight_row[indices]))
        rescaled_logits = outputs.astype(jnp.float32) * factor[:, None]
        return carry.at[indices].add(rescaled_logits), None

    total = jnp.zeros(tokens.shape, jnp.float32)
    total, unused = lax.scan(per_expert, total, (jnp.arange(EXPERTS, dtype=jnp.int32), gate_weight, up_weight, down_weight))
    return total.astype(jnp.bfloat16)
```

```python
import functools

import jax
import jax.numpy as jnp
from jax import lax
from jax.experimental import pallas as pl
from jax.experimental.pallas import tpu as pltpu
from jax.sharding import PartitionSpec as P

alpha_gate = 1.702
CHIPS_X = 4
CORES = 2
BF16 = jnp.bfloat16
F32 = jnp.float32
MESH = pl.DeviceIdType.MESH
LANES = 128


def log2(n):
    return n.bit_length() - 1


def layer_kernel(
    nx, nz, nc, cap, top, width,
    x_hbm, wg_hbm, wu_hbm, wd_hbm, o_ref,
    G, SEL, RECV, OUT, RET, PP, SW, CH, HID, wg, wu, wd,
    lsem, wsem, zs, zr, xs, xr, ys, yr, cs, cr,
):
    half = nz // 2
    plane = nx * nc
    tokens, padded = G.shape[2], G.shape[3]
    piece_rows = tokens // 2
    per = 2 * cap
    slots = plane * per
    meta_at = width - (padded - LANES)

    me = lax.axis_index("ep")
    core = lax.rem(me, nc)
    z = lax.rem(me // nc, nz)
    x = me // (nc * nz)
    seat = x * nc + core

    def device(x_, z_, c_):
        return {"ep": (x_ * nz + z_) * nc + c_}

    up = device(x, lax.rem(z + 1, nz), core)
    down = device(x, lax.rem(z + nz - 1, nz), core)
    ring = (up, down)
    seats = [lax.rem(seat + o, plane) for o in range(1, plane)]
    peers = [device(s // nc, z, lax.rem(s, nc)) for s in seats]

    loads = [
        pltpu.make_async_copy(
            x_hbm.at[pl.ds(i * piece_rows, piece_rows)],
            G.at[0, 0, pl.ds(i * piece_rows, piece_rows)],
            lsem.at[i],
        )
        for i in range(2)
    ]
    for load in loads:
        load.start()
    weight_loads = [
        pltpu.make_async_copy(src.at[0], dst, wsem.at[i])
        for i, (src, dst) in enumerate(((wg_hbm, wg), (wu_hbm, wu), (wd_hbm, wd)))
    ]
    for load in weight_loads:
        load.start()

    barrier = pltpu.get_barrier_semaphore()
    for peer in (*ring, *peers):
        pl.semaphore_signal(barrier, inc=1, device_id=peer, device_id_type=MESH)
    pl.semaphore_wait(barrier, len(ring) + len(peers))

    def hop(t, d, piece, last=False):
        rows = pl.ds(piece * piece_rows, piece_rows)
        src = G.at[t - 1, d, rows] if not isinstance(t, int) or t > 1 else G.at[0, 0, rows]
        dst = G.at[0, 1, rows] if last else G.at[t, d, rows]
        return pltpu.make_async_remote_copy(
            src_ref=src, dst_ref=dst, send_sem=zs.at[t, d, piece], recv_sem=zr.at[t, d, piece],
            device_id=ring[d], device_id_type=MESH,
        )

    def fan(src, dst, send, recv, p, i):
        at = pl.multiple_of(seats[i] * per, per)
        to = pl.multiple_of(seat * per, per)
        return pltpu.make_async_remote_copy(
            src_ref=src.at[p, pl.ds(at, per)], dst_ref=dst.at[p, pl.ds(to, per)],
            send_sem=send.at[p], recv_sem=recv.at[p], device_id=peers[i], device_id_type=MESH,
        )

    def fan_all(src, dst, send, recv, p):
        n = (plane - 1) * per
        return pltpu.make_async_remote_copy(
            src_ref=src.at[p, pl.ds(0, n)], dst_ref=dst.at[p, pl.ds(0, n)],
            send_sem=send.at[p], recv_sem=recv.at[p], device_id=peers[0], device_id_type=MESH,
        )

    def send_fan(src, dst, send, recv, p):
        for i in range(plane - 1):
            fan(src, dst, send, recv, p, i).start()
        mine = pl.ds(pl.multiple_of(seat * per, per), per)
        dst[p, mine] = src[p, mine]

    def select(p):
        lane = lax.broadcasted_iota(jnp.int32, (tokens, slots), 1)
        j = lane >> log2(per)
        side = (lane >> log2(cap)) & 1
        place = (lane & (cap - 1)).astype(F32)
        expert = (((j >> log2(nc)) * nz + z) * nc + (j & (nc - 1))).astype(F32)
        row = lax.broadcasted_iota(jnp.int32, (tokens, tokens), 0)
        col = lax.broadcasted_iota(jnp.int32, (tokens, tokens), 1)
        before = jnp.where(col < row, 1.0, 0.0).astype(BF16)
        picks = []
        for d in range(2):
            meta = G[p, d, :, padded - LANES :].astype(F32)
            on_side = jnp.where(side == d, expert, -1.0)
            hit = jnp.zeros((tokens, slots), F32)
            high = jnp.zeros((tokens, slots), F32)
            low = jnp.zeros((tokens, slots), F32)
            for k in range(top):
                at = meta_at + k
                same = meta[:, at : at + 1] == on_side
                hit = jnp.where(same, 1.0, hit)
                high = jnp.where(same, meta[:, at + top : at + top + 1], high)
                low = jnp.where(same, meta[:, at + 2 * top : at + 2 * top + 1], low)
            rank = jnp.dot(before, hit.astype(BF16), preferred_element_type=F32)
            keep = rank == place
            picks.append(jnp.where(keep, hit, 0.0).astype(BF16))
            SW[p, 0, d] = jnp.where(keep, high, 0.0).astype(BF16)
            SW[p, 1, d] = jnp.where(keep, low, 0.0).astype(BF16)
        pick = jnp.concatenate(picks, axis=0)
        blocks = jnp.concatenate([G[p, 0], G[p, 1]], axis=0)
        chosen = lax.dot_general(
            pick, blocks, (((0,), (0,)), ((), ())), preferred_element_type=F32
        )
        SEL[p] = chosen.astype(BF16)
        send_fan(SEL, RECV, xs, xr, p)

    def expert_in(p):
        fan_all(SEL, RECV, xs, xr, p).wait_recv()
        rows = RECV[p, :, :width]
        gate = jnp.dot(rows, wg[...], preferred_element_type=F32)
        up_part = jnp.dot(rows, wu[...], preferred_element_type=F32)
        HID[...] = ((up_part + 1.0) * gate * jax.nn.sigmoid(alpha_gate * gate)).astype(BF16)

    def expert_out(p):
        OUT[p, :, :width] = jnp.dot(HID[...], wd[...], preferred_element_type=F32).astype(BF16)
        send_fan(OUT, RET, ys, yr, p)

    def mix(p):
        fan_all(OUT, RET, ys, yr, p).wait_recv()
        answers = RET[p]
        for d in range(2):
            PP[p, d] = jnp.dot(SW[p, 0, d], answers, preferred_element_type=F32) + jnp.dot(
                SW[p, 1, d], answers, preferred_element_type=F32
            )

    for piece in range(2):
        loads[piece].wait()
        for d in range(2):
            hop(1, d, piece).start()

    def step(t, unused):
        @pl.when((t >= 1) & (t < half))
        def _():
            for d in range(2):
                hop(t, d, 1).wait_recv()

            @pl.when(t < half - 1)
            def _():
                for d in range(2):
                    hop(t + 1, d, 1).start()

            @pl.when(t == half - 1)
            def _():
                hop(t + 1, 1, 1, last=True).start()

        @pl.when(t == half)
        def _():
            hop(t, 1, 1, last=True).wait_recv()

        @pl.when((t >= 1) & (t <= half))
        def _():
            select(lax.rem(t, half))

        @pl.when(t == 2)
        def _():
            for load in weight_loads:
                load.wait()

        @pl.when((t >= 2) & (t <= half + 1))
        def _():
            expert_in(lax.rem(t - 1, half))

        @pl.when(t + 1 < half)
        def _():
            for d in range(2):
                hop(t + 1, d, 0).wait_recv()

            @pl.when(t + 2 < half)
            def _():
                for d in range(2):
                    hop(t + 2, d, 0).start()

            @pl.when(t + 2 == half)
            def _():
                hop(t + 2, 0, 0, last=True).start()

        @pl.when(t + 1 == half)
        def _():
            hop(t + 1, 0, 0, last=True).wait_recv()

        @pl.when((t >= 2) & (t <= half + 1))
        def _():
            expert_out(lax.rem(t - 1, half))

        @pl.when(t >= 3)
        def _():
            mix(lax.rem(t - 2, half))

        return unused

    lax.fori_loop(0, half + 2, step, 0)

    for t in range(1, half + 1):
        for d in range(2):
            for piece in range(2):
                if t < half or piece == d:
                    hop(t, d, piece, last=t == half).wait_send()

    def link(s, d, piece):
        rows = pl.ds(piece * piece_rows, piece_rows)
        return pltpu.make_async_remote_copy(
            src_ref=G.at[s, d, rows] if s < half else G.at[0, 1, rows],
            dst_ref=CH.at[d, s - 1, rows],
            send_sem=cs.at[s, d, piece], recv_sem=cr.at[s - 1, d, piece],
            device_id=ring[1 - d], device_id_type=MESH,
        )

    def pass_on(s, d, piece):
        rows = pl.ds(piece * piece_rows, piece_rows)
        at = (s, d) if s < half else (0, 1)
        total = PP[(*at, rows)]
        if s < half - 1 or (s == half - 1 and piece == d):
            link(s + 1, d, piece).wait_recv()
            total = total + CH[d, s, rows].astype(F32)
        G[(*at, rows)] = total.astype(BF16)
        link(s, d, piece).start()

    for d in range(2):
        pass_on(half - 1, d, 1 - d)
    mix(0)
    for i in range(half):
        for d in range(2):
            pass_on(half - i, d, d)
        if half - 2 - i >= 1:
            for d in range(2):
                pass_on(half - 2 - i, d, 1 - d)

    for piece in (1, 0):
        rows = pl.ds(piece * piece_rows, piece_rows)
        total = PP[0, 0, rows]
        for d in range(2):
            link(1, d, piece).wait_recv()
            total = total + CH[d, 0, rows].astype(F32)
        o_ref[rows] = total[:, :width].astype(BF16)

    for s in range(1, half + 1):
        for d in range(2):
            for piece in range(2):
                if s < half or piece == d:
                    link(s, d, piece).wait_send()
    for p in range(half):
        fan_all(SEL, RECV, xs, xr, p).wait_send()
        fan_all(OUT, RET, ys, yr, p).wait_send()


def on_device(nx, nc, tokens, expert_ids, combine, gate_weight, up_weight, down_weight):
    members = lax.axis_size("ep")
    nz = members // (nx * nc)
    half = nz // 2
    rows, width = tokens.shape
    top = expert_ids.shape[1]
    hidden = gate_weight.shape[2]
    cap = 2 * rows * top // members
    slots = nx * nc * 2 * cap
    high = lax.reduce_precision(combine, 8, 7)
    low = combine - high
    padded = -(-(width + 3 * top) // LANES) * LANES
    packed = jnp.concatenate(
        [
            tokens,
            expert_ids.astype(BF16),
            high.astype(BF16),
            low.astype(BF16),
            jnp.zeros((rows, padded - width - 3 * top), BF16),
        ],
        axis=1,
    )
    dma = pltpu.SemaphoreType.DMA
    any_space = pl.BlockSpec(memory_space=pl.ANY)
    return pl.pallas_call(
        functools.partial(layer_kernel, nx, nz, nc, cap, top, width),
        out_shape=jax.ShapeDtypeStruct((rows, width), BF16),
        in_specs=[any_space] * 4,
        out_specs=pl.BlockSpec(memory_space=pltpu.VMEM),
        scratch_shapes=[
            pltpu.VMEM((half, 2, rows, padded), BF16),
            pltpu.VMEM((half, slots, padded), BF16),
            pltpu.VMEM((half, slots, padded), BF16),
            pltpu.VMEM((half, slots, padded), BF16),
            pltpu.VMEM((half, slots, padded), BF16),
            pltpu.VMEM((half, 2, rows, padded), F32),
            pltpu.VMEM((half, 2, 2, rows, slots), BF16),
            pltpu.VMEM((2, half, rows, padded), BF16),
            pltpu.VMEM((slots, hidden), BF16),
            pltpu.VMEM((width, hidden), BF16),
            pltpu.VMEM((width, hidden), BF16),
            pltpu.VMEM((hidden, width), BF16),
            dma((2,)),
            dma((3,)),
            dma((half + 1, 2, 2)),
            dma((half + 1, 2, 2)),
            dma((half,)),
            dma((half,)),
            dma((half,)),
            dma((half,)),
            dma((half + 1, 2, 2)),
            dma((half + 1, 2, 2)),
        ],
        compiler_params=pltpu.CompilerParams(
            collective_id=0, has_side_effects=True, vmem_limit_bytes=67_043_328
        ),
        name="layer",
    )(packed, gate_weight, up_weight, down_weight)


def solution(mesh, nx=CHIPS_X, nc=CORES):
    in_specs = (
        P(("groups", "ep"), None),
        P(("groups", "ep"), None),
        P(("groups", "ep"), None),
        P("ep", None, None),
        P("ep", None, None),
        P("ep", None, None),
    )
    out_specs = P(("groups", "ep"), None)
    return jax.shard_map(
        functools.partial(on_device, nx, nc),
        mesh=mesh, in_specs=in_specs, out_specs=out_specs, check_vma=False,
    )
```
